32 devices in a mesh: row: 8 (over y, x, core), col: 4 (over z).
Axes of the slice: x: 2, y: 2, z: 4, core: 2. Of those that a mesh axis runs over, the one named last changes fastest.
Arguments:
- integrals: bfloat16 [320, 32, 4096], P('row', None, 'col'), may hold values from -6 to 6
- coeffs: bfloat16 [10240, 4096], P('row', 'col'), may hold values from -0.078125 to 0.078125
- mask: int32 [320, 4], replicated, may hold values from 0 to 1, as said below
- offsets: int32 [321], replicated, may hold values from 0 to 7680, as said below
- atom_of_slot: int32 [320], replicated, may hold values from 0 to 319, as said below
Outputs:
- half_transformed: bfloat16 [4096, 4096], P('row', 'col')
The draws below stay inside these ranges and needn't reach their ends.
Inputs may be any that keep to these rules, and one draw needn't show every extreme that they name: `mask`: 1 marks a significant pair of an atom and a block of 64 window functions. offsets[0] = 0 and offsets[a + 1] - offsets[a] is atom a's number of basis functions, 16 to 32; atoms 2k and 2k + 1 together have 3 * 16; rows of an atom's padded block past its number are padding. `atom_of_slot`: a permutation of the atoms; slot k is held by atom owner k // 40 along row, and atom a's AO-row owner is a // 40; one atom owner holds at least one and at most 5 atoms of any one AO-row owner, and exactly 5 for some pairs.
All inputs are finite; a program needn't handle non-finite values.
Results may differ from the reference program's by a relative error of at most 0.015.
Values may be sent and summed in bfloat16 or wider, within the bound.
A program may use at most 256 MiB of HBM per device.

```python
import jax
import jax.numpy as jnp
from jax import lax

AW = 32
ATOMS_DEV = 40
NOCC = 4096
NAUX = 16
NU_DEV = 64
NATOM = 320
NBAS = 10240
NU = 256
NVB = 4
CAP = 5
N_ROW = 8


def draw_mask(key, part):
    first_key = jax.random.fold_in(key, 11)
    second_key = jax.random.fold_in(key, 12)
    percent = jax.random.randint(first_key, (N_ROW,), 10, 96)
    rolled = jax.random.randint(second_key, (NATOM, NVB), 0, 100)
    owner = jnp.arange(NATOM, dtype=jnp.int32) // ATOMS_DEV
    return (rolled < percent[owner][:, None]).astype(jnp.int32)


def draw_offsets(key, part):
    firsts = jax.random.randint(jax.random.fold_in(key, 21), (NATOM // 2,), AW // 2, AW + 1)
    seconds = 3 * AW // 2 - firsts
    counts = jnp.stack([firsts, seconds], axis=1).reshape(-1).astype(jnp.int32)
    return jnp.concatenate([jnp.zeros((1,), jnp.int32), jnp.cumsum(counts).astype(jnp.int32)])


def draw_atom_of_slot(key, part):
    first_key = jax.random.fold_in(key, 31)
    second_key = jax.random.fold_in(key, 32)
    third_key = jax.random.fold_in(key, 33)
    fourth_key = jax.random.fold_in(key, 34)
    every_shift = jax.random.permutation(first_key, jnp.arange(N_ROW, dtype=jnp.int32))
    repeated = jnp.tile(jnp.arange(N_ROW, dtype=jnp.int32), CAP - 1)
    extra = jax.random.permutation(third_key, repeated)[:ATOMS_DEV - N_ROW]
    shifts = jax.random.permutation(fourth_key, jnp.concatenate([every_shift, extra]).astype(jnp.int32))
    locals_table = jax.vmap(lambda owner: jax.random.permutation(jax.random.fold_in(second_key, owner), ATOMS_DEV))(jnp.arange(N_ROW, dtype=jnp.int32))
    source = jnp.arange(N_ROW, dtype=jnp.int32)[:, None]
    layer = jnp.arange(ATOMS_DEV, dtype=jnp.int32)[None, :]
    target = (source - shifts[None, :]) % N_ROW
    chosen = locals_table[target, jnp.broadcast_to(layer, target.shape)].astype(jnp.int32)
    return (target * ATOMS_DEV + chosen).reshape(-1).astype(jnp.int32)


def strengthened(drawn, stream_key, source, target, parts, factor):
    def block_of(axis_at):
        return (jnp.arange(drawn.shape[axis_at]) // (drawn.shape[axis_at] // parts)).reshape((-1,) + (1,) * (drawn.ndim - 1 - axis_at))

    one_side = jax.random.permutation(stream_key, parts)[block_of(target)]
    second = (block_of(target) + parts // 2) % parts
    return jnp.where((block_of(source) == one_side) | (block_of(source) == second), factor * drawn, drawn)


def block_levels(rng, dims, split, smallest, largest):
    level = 1.0
    for position, shards_of in split:
        steps = jax.random.uniform(jax.random.fold_in(jax.random.fold_in(rng, 6), position), (shards_of,), jnp.float32, smallest / len(split), largest / len(split))
        level = level * jnp.repeat(jnp.exp(steps), dims[position] // shards_of).reshape((-1,) + (1,) * (len(dims) - 1 - position))
    return level


def normal_values(own_key, extent, spread, bound, shards=(), kind=jnp.bfloat16):
    result = spread * jax.random.normal(own_key, extent, jnp.float32)
    if shards:
        result = result * block_levels(own_key, extent, shards, -0.22, 0.18)
    return jnp.clip(result, -bound, bound).astype(kind)


def gaussian_with(rng, dims, scale, reach, cuts, heavy, held_as=jnp.bfloat16):
    drawn = scale * jax.random.normal(rng, dims, jnp.float32)
    if cuts:
        drawn = drawn * block_levels(rng, dims, cuts, -0.22, 0.18)
    return jnp.clip(strengthened(drawn, jax.random.fold_in(rng, 3), *heavy), -reach, reach).astype(held_as)


def setup_inputs(seed: int = 0) -> dict:
    key_list = jax.random.split(jax.random.key(seed), 6)
    return {
        "integrals": normal_values(key_list[0], (NATOM, AW, NU * NAUX), 1.0, 6.0, ((0, 8), (2, 4))),
        "coeffs": gaussian_with(key_list[1], (NBAS, NOCC), NBAS ** -0.5, 0.078125, ((0, 8), (1, 4)), (0, 1, 8, 2.0)),
        "mask": draw_mask(jax.random.fold_in(key_list[5], 71), 0),
        "offsets": draw_offsets(jax.random.fold_in(key_list[5], 71), 0),
        "atom_of_slot": draw_atom_of_slot(jax.random.fold_in(key_list[5], 71), 0),
    }


def reference(integrals, coeffs, mask, offsets, atom_of_slot):
    natoms = integrals.shape[0]
    inverse = jnp.zeros((natoms,), jnp.int32).at[atom_of_slot].set(jnp.arange(natoms, dtype=jnp.int32))
    ordered = integrals[inverse]
    lengths = offsets[1:] - offsets[:-1]
    row_live = (jnp.arange(AW, dtype=jnp.int32)[None, :] < lengths[:, None]).astype(jnp.bfloat16)
    column_live = jnp.repeat(mask, NU_DEV * NAUX, axis=1).astype(jnp.bfloat16)
    kept = ordered * row_live[:, :, None] * column_live[:, None, :]
    width = kept.shape[2]
    kept_groups = kept.reshape(N_ROW, ATOMS_DEV * AW, width)
    coeff_groups = coeffs.reshape(N_ROW, ATOMS_DEV * AW, coeffs.shape[1])

    def add_owner(total, pieces):
        coeff_piece, kept_piece = pieces
        part = lax.dot_general(coeff_piece, kept_piece, (((0,), (0,)), ((), ())), preferred_element_type=jnp.float32)
        part = lax.optimization_barrier(part.astype(jnp.bfloat16))
        return total + part.astype(jnp.float32), None

    start = jnp.zeros((coeffs.shape[1], width), jnp.float32)
    half, unused = lax.scan(add_owner, start, (coeff_groups, kept_groups))
    return half.astype(jnp.bfloat16)
```

```python
import functools

import jax
import jax.numpy as jnp
from jax import lax
from jax.experimental import pallas as pl
from jax.experimental.pallas import tpu as pltpu
from jax.sharding import PartitionSpec as P

MESH = pl.DeviceIdType.MESH
F32 = jnp.float32
BF16 = jnp.bfloat16


def remote(src, dst, send, recv, device):
    return pltpu.make_async_remote_copy(
        src_ref=src, dst_ref=dst, send_sem=send, recv_sem=recv, device_id=device, device_id_type=MESH
    )


def nearest(me, n, s):
    m = jnp.minimum(me, n - 1 - me)
    step = (s + 1) // 2
    near = jnp.where(s % 2 == 1, me - step, me + step)
    far = jnp.where(me <= n - 1 - me, s, n - 1 - s)
    return jnp.where(s <= 2 * m, near, far)


def kernel(
    n_row, n_col, cap, chunks, width,
    meta, integrals, coeffs, out,
    asend, arecv, kept, gathered, mine1, send1, recv1, sums,
    a_ss, a_rs, r_ss, l_ss, g_rs, s1_ss, s1_rs, s2_ss, s2_rs,
):
    me = lax.axis_index("row")
    plane = lax.axis_index("col")
    core = me % 2
    chip = me // 2
    n_chip = n_row // 2
    partner = me + 1 - 2 * core
    per_dev, atom_w, row_width = integrals.shape
    half = atom_w // 2
    pairs = per_dev // 2
    packed = 3 * half
    slots = n_row * cap
    per_plane = n_row // n_col
    chips_plane = per_plane // 2
    block = width * chunks
    pick0, len0, sig0 = slots, slots + per_dev, slots + 2 * per_dev
    has_left = plane > 0
    has_right = plane < n_col - 1

    barrier = pltpu.get_barrier_semaphore()
    for other in range(1, n_row):
        pl.semaphore_signal(barrier, inc=1, device_id=((me + other) % n_row, plane), device_id_type=MESH)

    @pl.when(has_left)
    def _():
        pl.semaphore_signal(barrier, inc=1, device_id=(me, plane - 1), device_id_type=MESH)

    @pl.when(has_right)
    def _():
        pl.semaphore_signal(barrier, inc=1, device_id=(me, plane + 1), device_id_type=MESH)

    def selection(p, weighted):
        s = lax.broadcasted_iota(jnp.int32, (packed, 2 * atom_w), 0)
        t = lax.broadcasted_iota(jnp.int32, (packed, 2 * atom_w), 1)
        extra = meta[len0 + 2 * p] - half
        source = jnp.where(
            s < half, s, jnp.where(s < 2 * half, s + half, jnp.where(s - 2 * half < extra, s - half, s + half - extra))
        )
        hit = source == t
        if weighted:
            sig = jnp.where(t < atom_w, meta[sig0 + 2 * p], meta[sig0 + 2 * p + 1])
            hit = hit & (sig > 0)
        return jnp.where(hit, 1.0, 0.0).astype(BF16)

    def pack_coeffs(p, carry):
        rows = coeffs[pl.ds(pl.multiple_of(p * 2 * atom_w, 2 * atom_w), 2 * atom_w), :]
        live = jnp.dot(selection(p, False), rows, preferred_element_type=F32).astype(BF16)
        at = pl.ds(pl.multiple_of(p * packed, 16), packed)
        for k in range(chunks):
            for b in range(per_plane):
                lo = b * block + k * width
                gathered[plane, k, at, b * width : (b + 1) * width] = live[:, lo : lo + width]
        return carry

    lax.fori_loop(0, pairs, pack_coeffs, 0)
    pl.semaphore_wait(barrier, n_row - 1 + has_left.astype(jnp.int32) + has_right.astype(jnp.int32))

    def to_right(z, k):
        return remote(gathered.at[z, k], gathered.at[z, k], r_ss.at[z, k], g_rs.at[z, k], (me, plane + 1))

    def to_left(z, k):
        return remote(gathered.at[z, k], gathered.at[z, k], l_ss.at[z, k], g_rs.at[z, k], (me, plane - 1))

    def forward(z, k):
        @pl.when((z <= plane) & has_right)
        def _():
            to_right(z, k).start()

        @pl.when((z >= plane) & has_left)
        def _():
            to_left(z, k).start()

    for k in range(chunks):
        forward(plane, k)

    def a_copy(owner):
        return remote(asend.at[owner], arecv.at[me], a_ss.at[owner], a_rs.at[me], (owner, plane))

    def place(step, carry):
        owner = (me + step) % n_row

        @pl.when(step > 0)
        def _():
            for c in range(cap):
                asend[owner, c] = integrals[meta[owner * cap + c]]
            a_copy(owner).start()

        @pl.when(step == 0)
        def _():
            for c in range(cap):
                arecv[me, c] = integrals[meta[me * cap + c]]

        return carry

    lax.fori_loop(0, n_row, place, 0)

    def wait_blocks(step, carry):
        source = (me + step) % n_row
        remote(asend.at[source], arecv.at[source], a_ss.at[source], a_rs.at[source], (source, plane)).wait_recv()
        return carry

    lax.fori_loop(1, n_row, wait_blocks, 0)

    def pack_kept(p, carry):
        first, second = meta[pick0 + 2 * p], meta[pick0 + 2 * p + 1]
        rows = jnp.concatenate([arecv[first // cap, first % cap], arecv[second // cap, second % cap]], axis=0)
        live = jnp.dot(selection(p, True), rows, preferred_element_type=F32).astype(BF16)
        kept[pl.ds(pl.multiple_of(p * packed, 16), packed), :] = live
        return carry

    lax.fori_loop(0, pairs, pack_kept, 0)

    def core_copy(z, k):
        return remote(send1.at[z, k], recv1.at[z, k], s1_ss.at[z, k], s1_rs.at[z, k], (partner, plane))

    def chip_copy(target, k):
        return remote(
            mine1.at[target, k], sums.at[chip, k], s2_ss.at[target, k], s2_rs.at[chip, k], (2 * target + core, plane)
        )

    total = n_col * chunks

    def step_body(n, carry):
        @pl.when(n < total)
        def _():
            z = nearest(plane, n_col, n // chunks)
            k = n % chunks

            @pl.when(z != plane)
            def _():
                to_right(z, k).wait_recv()
                forward(z, k)

            part = lax.dot_general(
                gathered[z, k], kept[...], (((0,), (0,)), ((), ())), preferred_element_type=F32
            ).astype(BF16)
            for j in range(chips_plane):
                lower = part[2 * j * width : (2 * j + 1) * width]
                upper = part[(2 * j + 1) * width : (2 * j + 2) * width]
                is_lower = core == 0
                mine1[z * chips_plane + j, k] = jnp.where(is_lower, lower, upper)
                send1[z, k, j] = jnp.where(is_lower, upper, lower)
            core_copy(z, k).start()

        @pl.when(n > 0)
        def _():
            z = nearest(plane, n_col, (n - 1) // chunks)
            k = (n - 1) % chunks
            core_copy(z, k).wait_recv()
            for j in range(chips_plane):
                target = z * chips_plane + j
                both = mine1[target, k].astype(F32) + recv1[z, k, j].astype(F32)

                @pl.when(target == chip)
                def _():
                    sums[target, k] = both.astype(BF16)

                @pl.when(target != chip)
                def _():
                    mine1[target, k] = both.astype(BF16)
                    chip_copy(target, k).start()

        return carry

    lax.fori_loop(0, total + 1, step_body, 0)

    for k in range(chunks):

        def wait_sums(step, carry):
            source = (chip + step) % n_chip
            remote(
                mine1.at[source, k], sums.at[source, k], s2_ss.at[source, k], s2_rs.at[source, k],
                (2 * source + core, plane),
            ).wait_recv()
            return carry

        lax.fori_loop(1, n_chip, wait_sums, 0)
        acc = sums[0, k].astype(F32)
        for q in range(1, n_chip):
            acc += sums[q, k].astype(F32)
        out[k * width : (k + 1) * width, :] = acc.astype(BF16)

    def drain_blocks(step, carry):
        a_copy((me + step) % n_row).wait_send()
        return carry

    lax.fori_loop(1, n_row, drain_blocks, 0)

    def drain(n, carry):
        z, k = n // chunks, n % chunks
        core_copy(z, k).wait_send()

        @pl.when((z <= plane) & has_right)
        def _():
            to_right(z, k).wait_send()

        @pl.when((z >= plane) & has_left)
        def _():
            to_left(z, k).wait_send()

        for j in range(chips_plane):
            target = z * chips_plane + j

            @pl.when(target != chip)
            def _():
                chip_copy(target, k).wait_send()

        return carry

    lax.fori_loop(0, total, drain, 0)


def body(integrals, coeffs, mask, offsets, atom_of_slot):
    n_row = lax.axis_size("row")
    n_col = lax.axis_size("col")
    me = lax.axis_index("row")
    plane = lax.axis_index("col")
    per_dev, atom_w, row_width = integrals.shape
    rows, cols = coeffs.shape
    cap = max(2, -(-per_dev // n_row))
    slots = n_row * cap
    block = cols * n_col // n_row
    chunks = max(1, min(4, block // 128))
    width = block // chunks
    per_plane = n_row // n_col

    holders = atom_of_slot.reshape(n_row, per_dev)
    slot = jnp.arange(per_dev, dtype=jnp.int32)
    mine = lax.dynamic_slice_in_dim(atom_of_slot, me * per_dev, per_dev)
    owner = mine // per_dev
    before = (owner[None, :] == owner[:, None]) & (slot[None, :] < slot[:, None])
    position = owner * cap + jnp.sum(before.astype(jnp.int32), axis=1)
    order = jnp.sum(
        jnp.where(jnp.arange(slots, dtype=jnp.int32)[:, None] == position[None, :], slot[None, :], 0), axis=1
    )
    is_mine = holders // per_dev == me
    earlier = is_mine[:, None, :] & (slot[None, None, :] < slot[None, :, None])
    arrival = jnp.sum(earlier.astype(jnp.int32), axis=2)
    place = (jnp.arange(n_row, dtype=jnp.int32)[:, None] * cap + arrival).reshape(-1)
    pick = jnp.sum(
        jnp.where((me * per_dev + slot)[:, None] == atom_of_slot[None, :], place[None, :], 0), axis=1
    )
    bounds = lax.dynamic_slice_in_dim(offsets, me * per_dev, per_dev + 1)
    lengths = bounds[1:] - bounds[:-1]
    significant = lax.dynamic_slice(mask, (me * per_dev, plane), (per_dev, 1))[:, 0]
    meta = jnp.concatenate([order, pick, lengths, significant])

    packed = rows * 3 // 4
    dma = pltpu.SemaphoreType.DMA
    n_chip = n_row // 2
    pair_width = per_plane * width
    return pl.pallas_call(
        functools.partial(kernel, n_row, n_col, cap, chunks, width),
        out_shape=jax.ShapeDtypeStruct((block, row_width), BF16),
        in_specs=[pl.BlockSpec(memory_space=pltpu.SMEM)] + [pl.BlockSpec(memory_space=pltpu.VMEM)] * 2,
        out_specs=pl.BlockSpec(memory_space=pltpu.VMEM),
        scratch_shapes=[
            pltpu.VMEM((n_row, cap, atom_w, row_width), BF16),
            pltpu.VMEM((n_row, cap, atom_w, row_width), BF16),
            pltpu.VMEM((packed, row_width), BF16),
            pltpu.VMEM((n_col, chunks, packed, pair_width), BF16),
            pltpu.VMEM((n_chip, chunks, width, row_width), BF16),
            pltpu.VMEM((n_col, chunks, per_plane // 2, width, row_width), BF16),
            pltpu.VMEM((n_col, chunks, per_plane // 2, width, row_width), BF16),
            pltpu.VMEM((n_chip, chunks, width, row_width), BF16),
            dma((n_row,)),
            dma((n_row,)),
            dma((n_col, chunks)),
            dma((n_col, chunks)),
            dma((n_col, chunks)),
            dma((n_col, chunks)),
            dma((n_col, chunks)),
            dma((n_chip, chunks)),
            dma((n_chip, chunks)),
        ],
        compiler_params=pltpu.CompilerParams(
            collective_id=0, has_side_effects=True, vmem_limit_bytes=62 << 20
        ),
    )(meta, integrals, coeffs)


def solution(mesh):
    in_specs = (P("row", None, "col"), P("row", "col"), P(), P(), P())
    out_specs = P("row", "col")
    return jax.shard_map(body, mesh=mesh, in_specs=in_specs, out_specs=out_specs, check_vma=False)
```

```python
import functools

import jax
import jax.numpy as jnp
from jax import lax
from jax.experimental import pallas as pl
from jax.experimental.pallas import tpu as pltpu
from jax.sharding import PartitionSpec as P

MESH = pl.DeviceIdType.MESH
F32 = jnp.float32
BF16 = jnp.bfloat16


def remote(src, dst, send, recv, device):
    return pltpu.make_async_remote_copy(
        src_ref=src, dst_ref=dst, send_sem=send, recv_sem=recv, device_id=device, device_id_type=MESH
    )


def nearest(me, n, s):
    m = jnp.minimum(me, n - 1 - me)
    step = (s + 1) // 2
    near = jnp.where(s % 2 == 1, me - step, me + step)
    far = jnp.where(me <= n - 1 - me, s, n - 1 - s)
    return jnp.where(s <= 2 * m, near, far)


def kernel(
    n_row, n_col, cap, chunks, width,
    meta, integrals, coeffs, out,
    asend, arecv, kept, gathered, mine1, send1, recv1, sums, kept_end, mine4, send4, recv4,
    a_ss, a_rs, r_ss, l_ss, g_rs, s1_ss, s1_rs, s2_ss, s2_rs, k_ss, k_rs, s4_ss, s4_rs, s3_ss, s3_rs,
):
    me = lax.axis_index("row")
    plane = lax.axis_index("col")
    core = me % 2
    chip = me // 2
    n_chip = n_row // 2
    partner = me + 1 - 2 * core
    per_dev, atom_w, row_width = integrals.shape
    half = atom_w // 2
    pairs = per_dev // 2
    packed = 3 * half
    slots = n_row * cap
    per_plane = n_row // n_col
    chips_plane = per_plane // 2
    block = width * chunks
    pick0, len0, sig0 = slots, slots + per_dev, slots + 2 * per_dev
    has_left = plane > 0
    has_right = plane < n_col - 1

    share = n_col >= 4
    pieces = chunks
    piece = row_width // pieces
    is_end = ((plane == 0) | (plane == n_col - 1)) & share
    is_helper = ((plane == 1) | (plane == n_col - 2)) & share
    low_half = plane <= n_col - 1 - plane
    end_plane = jnp.where(low_half, 0, n_col - 1)
    helper_plane = jnp.where(low_half, 1, n_col - 2)
    mate_plane = jnp.where(is_end, helper_plane, end_plane)

    barrier = pltpu.get_barrier_semaphore()
    for other in range(1, n_row):
        pl.semaphore_signal(barrier, inc=1, device_id=((me + other) % n_row, plane), device_id_type=MESH)

    @pl.when(has_left)
    def _():
        pl.semaphore_signal(barrier, inc=1, device_id=(me, plane - 1), device_id_type=MESH)

    @pl.when(has_right)
    def _():
        pl.semaphore_signal(barrier, inc=1, device_id=(me, plane + 1), device_id_type=MESH)

    @pl.when(is_end | is_helper)
    def _():
        def greet(step, carry):
            mate = 2 * ((chip + step) % n_chip) + core
            pl.semaphore_signal(barrier, inc=1, device_id=(mate, mate_plane), device_id_type=MESH)
            return carry

        lax.fori_loop(1, n_chip, greet, 0)

    def selection(p, weighted):
        s = lax.broadcasted_iota(jnp.int32, (packed, 2 * atom_w), 0)
        t = lax.broadcasted_iota(jnp.int32, (packed, 2 * atom_w), 1)
        extra = meta[len0 + 2 * p] - half
        source = jnp.where(
            s < half, s, jnp.where(s < 2 * half, s + half, jnp.where(s - 2 * half < extra, s - half, s + half - extra))
        )
        hit = source == t
        if weighted:
            sig = jnp.where(t < atom_w, meta[sig0 + 2 * p], meta[sig0 + 2 * p + 1])
            hit = hit & (sig > 0)
        return jnp.where(hit, 1.0, 0.0).astype(BF16)

    def pack_coeffs(p, carry):
        rows = coeffs[pl.ds(pl.multiple_of(p * 2 * atom_w, 2 * atom_w), 2 * atom_w), :]
        live = jnp.dot(selection(p, False), rows, preferred_element_type=F32).astype(BF16)
        at = pl.ds(pl.multiple_of(p * packed, 16), packed)
        for k in range(chunks):
            for b in range(per_plane):
                lo = b * block + k * width
                gathered[plane, k, at, b * width : (b + 1) * width] = live[:, lo : lo + width]
        return carry

    lax.fori_loop(0, pairs, pack_coeffs, 0)
    extra_mates = jnp.where(is_end | is_helper, n_chip - 1, 0)
    pl.semaphore_wait(barrier, n_row - 1 + has_left.astype(jnp.int32) + has_right.astype(jnp.int32) + extra_mates)

    def to_right(z, k):
        return remote(gathered.at[z, k], gathered.at[z, k], r_ss.at[z, k], g_rs.at[z, k], (me, plane + 1))

    def to_left(z, k):
        return remote(gathered.at[z, k], gathered.at[z, k], l_ss.at[z, k], g_rs.at[z, k], (me, plane - 1))

    def goes_right(z):
        ok = (z <= plane) & has_right
        return ok & ((plane != n_col - 2) | (z == plane)) if share else ok

    def goes_left(z):
        ok = (z >= plane) & has_left
        return ok & ((plane != 1) | (z == plane)) if share else ok

    def forward(z, k):
        @pl.when(goes_right(z))
        def _():
            to_right(z, k).start()

        @pl.when(goes_left(z))
        def _():
            to_left(z, k).start()

    for k in range(chunks):
        forward(plane, k)

    def a_copy(owner):
        return remote(asend.at[owner], arecv.at[me], a_ss.at[owner], a_rs.at[me], (owner, plane))

    def place(step, carry):
        owner = (me + step) % n_row

        @pl.when(step > 0)
        def _():
            for c in range(cap):
                asend[owner, c] = integrals[meta[owner * cap + c]]
            a_copy(owner).start()

        @pl.when(step == 0)
        def _():
            for c in range(cap):
                arecv[me, c] = integrals[meta[me * cap + c]]

        return carry

    lax.fori_loop(0, n_row, place, 0)

    def wait_blocks(step, carry):
        source = (me + step) % n_row
        remote(asend.at[source], arecv.at[source], a_ss.at[source], a_rs.at[source], (source, plane)).wait_recv()
        return carry

    lax.fori_loop(1, n_row, wait_blocks, 0)

    def pack_kept(p, carry):
        first, second = meta[pick0 + 2 * p], meta[pick0 + 2 * p + 1]
        rows = jnp.concatenate([arecv[first // cap, first % cap], arecv[second // cap, second % cap]], axis=0)
        live = jnp.dot(selection(p, True), rows, preferred_element_type=F32).astype(BF16)
        kept[pl.ds(pl.multiple_of(p * packed, 16), packed), :] = live
        return carry

    lax.fori_loop(0, pairs, pack_kept, 0)

    def piece_at(q):
        return pl.ds(pl.multiple_of(q * piece, 128), piece)

    def kept_copy(q):
        return remote(
            kept.at[:, piece_at(q)], kept_end.at[:, piece_at(q)], k_ss.at[q], k_rs.at[q], (me, helper_plane)
        )

    if share:

        @pl.when(is_end)
        def _():
            for q in range(pieces):
                kept_copy(q).start()

    def core_copy(z, k):
        return remote(send1.at[z, k], recv1.at[z, k], s1_ss.at[z, k], s1_rs.at[z, k], (partner, plane))

    def chip_copy(target, k):
        return remote(
            mine1.at[target, k], sums.at[chip, k], s2_ss.at[target, k], s2_rs.at[chip, k], (2 * target + core, plane)
        )

    steps = jnp.where(is_end, 2 * chunks, n_col * chunks)

    def finish(n):
        z = nearest(plane, n_col, n // chunks)
        k = n % chunks
        core_copy(z, k).wait_recv()
        for j in range(chips_plane):
            target = z * chips_plane + j
            both = mine1[target, k].astype(F32) + recv1[z, k, j].astype(F32)

            @pl.when(target == chip)
            def _():
                sums[target, k] = both.astype(BF16)

            @pl.when(target != chip)
            def _():
                mine1[target, k] = both.astype(BF16)
                chip_copy(target, k).start()

    near = (n_col - 3) * chunks

    def begin(t):
        return near * t + t * t

    def decode(e):
        e = jnp.asarray(e, jnp.int32)
        t = jnp.int32(0)
        for w in range(1, chunks):
            t += (e >= begin(w)).astype(jnp.int32)
        u = e - begin(t)
        last = u >= near
        v = u - near
        early = v <= t
        far = jnp.where(last, n_col - 3, u // chunks)
        k = jnp.where(last, jnp.where(early, v, t), u % chunks)
        q = jnp.where(last & (v > t), v - 1 - t, t)
        z = jnp.where(low_half, far + 2, n_col - 3 - far)
        return far, z, k, q

    def far_core_copy(far, k, q):
        return remote(
            send4.at[far, k, q], recv4.at[far, k, q], s4_ss.at[far, k, q], s4_rs.at[far, k, q], (partner, plane)
        )

    def far_copy(far, z, j, k, q):
        target = z * chips_plane + j
        return remote(
            mine4.at[far, k, q, j], sums.at[chip, k, :, piece_at(q)], s3_ss.at[target, k, q], s3_rs.at[chip, k, q],
            (2 * target + core, end_plane),
        )

    def far_start(e):
        far, z, k, q = decode(e)

        part = lax.dot_general(
            gathered[z, k], kept_end[:, piece_at(q)], (((0,), (0,)), ((), ())), preferred_element_type=F32
        ).astype(BF16)
        for j in range(chips_plane):
            lower = part[2 * j * width : (2 * j + 1) * width]
            upper = part[(2 * j + 1) * width : (2 * j + 2) * width]
            is_lower = core == 0
            mine4[far, k, q, j] = jnp.where(is_lower, lower, upper)
            send4[far, k, q, j] = jnp.where(is_lower, upper, lower)
        far_core_copy(far, k, q).start()

    def far_finish(e):
        far, z, k, q = decode(e)
        far_core_copy(far, k, q).wait_recv()
        for j in range(chips_plane):
            both = mine4[far, k, q, j].astype(F32) + recv4[far, k, q, j].astype(F32)
            mine4[far, k, q, j] = both.astype(BF16)
            far_copy(far, z, j, k, q).start()

    def step_body(n, carry):
        @pl.when(n < steps)
        def _():
            z = nearest(plane, n_col, n // chunks)
            k = n % chunks

            @pl.when(z != plane)
            def _():
                to_right(z, k).wait_recv()
                forward(z, k)

            part = lax.dot_general(
                gathered[z, k], kept[...], (((0,), (0,)), ((), ())), preferred_element_type=F32
            ).astype(BF16)
            for j in range(chips_plane):
                lower = part[2 * j * width : (2 * j + 1) * width]
                upper = part[(2 * j + 1) * width : (2 * j + 2) * width]
                is_lower = core == 0
                mine1[z * chips_plane + j, k] = jnp.where(is_lower, lower, upper)
                send1[z, k, j] = jnp.where(is_lower, upper, lower)
            core_copy(z, k).start()

        @pl.when(n > 0)
        def _():
            finish(n - 1)

        if share:
            t = n - (n_col - 1) * chunks

            @pl.when(is_helper & (t >= 0) & (t < chunks))
            def _():
                kept_copy(t).wait_recv()

                def far_body(e, carry):
                    far_start(e)

                    @pl.when(e > 0)
                    def _():
                        far_finish(e - 1)

                    return carry

                lax.fori_loop(begin(t), begin(t + 1), far_body, 0)

        return carry

    lax.fori_loop(0, steps + 1, step_body, 0)
    if share:

        @pl.when(is_helper)
        def _():
            far_finish(begin(chunks) - 1)

    my_plane = chip // chips_plane
    distance = jnp.where(low_half, my_plane, n_col - 1 - my_plane)
    from_helper = is_end & (distance >= 2)

    @pl.when(jnp.logical_not(from_helper))
    def _():
        def wait_sums(step, carry):
            source = (chip + step) % n_chip
            for k in range(chunks):
                remote(
                    mine1.at[source, k], sums.at[source, k], s2_ss.at[source, k], s2_rs.at[source, k],
                    (2 * source + core, plane),
                ).wait_recv()
            return carry

        lax.fori_loop(1, n_chip, wait_sums, 0)

    if share:

        @pl.when(from_helper)
        def _():
            def wait_far(source, carry):
                for k in range(chunks):
                    for q in range(pieces):
                        remote(
                            mine4.at[0, k, q, 0], sums.at[source, k, :, piece_at(q)], s3_ss.at[source, k, q],
                            s3_rs.at[source, k, q], (2 * source + core, helper_plane),
                        ).wait_recv()
                return carry

            lax.fori_loop(0, n_chip, wait_far, 0)

    for k in range(chunks):
        acc = sums[0, k].astype(F32)
        for q in range(1, n_chip):
            acc += sums[q, k].astype(F32)
        out[k * width : (k + 1) * width, :] = acc.astype(BF16)

    def drain_blocks(step, carry):
        a_copy((me + step) % n_row).wait_send()
        return carry

    lax.fori_loop(1, n_row, drain_blocks, 0)

    def drain(n, carry):
        z, k = nearest(plane, n_col, n // chunks), n % chunks
        core_copy(z, k).wait_send()

        @pl.when(goes_right(z))
        def _():
            to_right(z, k).wait_send()

        @pl.when(goes_left(z))
        def _():
            to_left(z, k).wait_send()

        for j in range(chips_plane):
            target = z * chips_plane + j

            @pl.when(target != chip)
            def _():
                chip_copy(target, k).wait_send()

        return carry

    lax.fori_loop(0, steps, drain, 0)
    if share:

        @pl.when(is_end)
        def _():
            for q in range(pieces):
                kept_copy(q).wait_send()

        @pl.when(is_helper)
        def _():
            def drain_far(e, carry):
                far, z, k, q = decode(e)
                far_core_copy(far, k, q).wait_send()
                for j in range(chips_plane):
                    far_copy(far, z, j, k, q).wait_send()
                return carry

            lax.fori_loop(0, begin(chunks), drain_far, 0)


def body(integrals, coeffs, mask, offsets, atom_of_slot):
    n_row = lax.axis_size("row")
    n_col = lax.axis_size("col")
    me = lax.axis_index("row")
    plane = lax.axis_index("col")
    per_dev, atom_w, row_width = integrals.shape
    rows, cols = coeffs.shape
    cap = max(2, -(-per_dev // n_row))
    slots = n_row * cap
    block = cols * n_col // n_row
    chunks = max(1, min(4, block // 128))
    width = block // chunks
    per_plane = n_row // n_col

    holders = atom_of_slot.reshape(n_row, per_dev)
    slot = jnp.arange(per_dev, dtype=jnp.int32)
    mine = lax.dynamic_slice_in_dim(atom_of_slot, me * per_dev, per_dev)
    owner = mine // per_dev
    before = (owner[None, :] == owner[:, None]) & (slot[None, :] < slot[:, None])
    position = owner * cap + jnp.sum(before.astype(jnp.int32), axis=1)
    order = jnp.sum(
        jnp.where(jnp.arange(slots, dtype=jnp.int32)[:, None] == position[None, :], slot[None, :], 0), axis=1
    )
    is_mine = holders // per_dev == me
    earlier = is_mine[:, None, :] & (slot[None, None, :] < slot[None, :, None])
    arrival = jnp.sum(earlier.astype(jnp.int32), axis=2)
    place = (jnp.arange(n_row, dtype=jnp.int32)[:, None] * cap + arrival).reshape(-1)
    pick = jnp.sum(
        jnp.where((me * per_dev + slot)[:, None] == atom_of_slot[None, :], place[None, :], 0), axis=1
    )
    bounds = lax.dynamic_slice_in_dim(offsets, me * per_dev, per_dev + 1)
    lengths = bounds[1:] - bounds[:-1]
    significant = lax.dynamic_slice(mask, (me * per_dev, plane), (per_dev, 1))[:, 0]
    meta = jnp.concatenate([order, pick, lengths, significant])

    packed = rows * 3 // 4
    dma = pltpu.SemaphoreType.DMA
    n_chip = n_row // 2
    pair_width = per_plane * width
    n_far = max(1, n_col - 2)
    far_shape = (n_far, chunks, chunks, per_plane // 2, width, row_width // chunks)
    return pl.pallas_call(
        functools.partial(kernel, n_row, n_col, cap, chunks, width),
        out_shape=jax.ShapeDtypeStruct((block, row_width), BF16),
        in_specs=[pl.BlockSpec(memory_space=pltpu.SMEM)] + [pl.BlockSpec(memory_space=pltpu.VMEM)] * 2,
        out_specs=pl.BlockSpec(memory_space=pltpu.VMEM),
        scratch_shapes=[
            pltpu.VMEM((n_row, cap, atom_w, row_width), BF16),
            pltpu.VMEM((n_row, cap, atom_w, row_width), BF16),
            pltpu.VMEM((packed, row_width), BF16),
            pltpu.VMEM((n_col, chunks, packed, pair_width), BF16),
            pltpu.VMEM((n_chip, chunks, width, row_width), BF16),
            pltpu.VMEM((n_col, chunks, per_plane // 2, width, row_width), BF16),
            pltpu.VMEM((n_col, chunks, per_plane // 2, width, row_width), BF16),
            pltpu.VMEM((n_chip, chunks, width, row_width), BF16),
            pltpu.VMEM((packed, row_width), BF16),
            pltpu.VMEM(far_shape, BF16),
            pltpu.VMEM(far_shape, BF16),
            pltpu.VMEM(far_shape, BF16),
            dma((n_row,)),
            dma((n_row,)),
            dma((n_col, chunks)),
            dma((n_col, chunks)),
            dma((n_col, chunks)),
            dma((n_col, chunks)),
            dma((n_col, chunks)),
            dma((n_chip, chunks)),
            dma((n_chip, chunks)),
            dma((chunks,)),
            dma((chunks,)),
            dma((n_far, chunks, chunks)),
            dma((n_far, chunks, chunks)),
            dma((n_chip, chunks, chunks)),
            dma((n_chip, chunks, chunks)),
        ],
        compiler_params=pltpu.CompilerParams(
            collective_id=0, has_side_effects=True, vmem_limit_bytes=62 << 20
        ),
    )(meta, integrals, coeffs)


def solution(mesh):
    in_specs = (P("row", None, "col"), P("row", "col"), P(), P(), P())
    out_specs = P("row", "col")
    return jax.shard_map(body, mesh=mesh, in_specs=in_specs, out_specs=out_specs, check_vma=False)
```

```python
import functools

import jax
import jax.numpy as jnp
from jax import lax
from jax.experimental import pallas as pl
from jax.experimental.pallas import tpu as pltpu
from jax.sharding import PartitionSpec as P

MESH = pl.DeviceIdType.MESH
F32 = jnp.float32
BF16 = jnp.bfloat16


def remote(src, dst, send, recv, device):
    return pltpu.make_async_remote_copy(
        src_ref=src, dst_ref=dst, send_sem=send, recv_sem=recv, device_id=device, device_id_type=MESH
    )


def nearest(me, n, s):
    m = jnp.minimum(me, n - 1 - me)
    step = (s + 1) // 2
    near = jnp.where(s % 2 == 1, me - step, me + step)
    far = jnp.where(me <= n - 1 - me, s, n - 1 - s)
    return jnp.where(s <= 2 * m, near, far)


def kernel(
    n_row, n_col, cap, chunks, width,
    meta, integrals, coeffs, out,
    asend, arecv, kept, gathered, mine1, send1, recv1, sums, kept_end, mine4, send4, recv4, relay,
    a_ss, a_rs, r_ss, l_ss, g_rs, s1_ss, s1_rs, s2_ss, s2_rs, k_ss, k_rs, s4_ss, s4_rs, s3_ss, s3_rs, s5_ss, s5_rs,
):
    me = lax.axis_index("row")
    plane = lax.axis_index("col")
    core = me % 2
    chip = me // 2
    n_chip = n_row // 2
    partner = me + 1 - 2 * core
    per_dev, atom_w, row_width = integrals.shape
    half = atom_w // 2
    pairs = per_dev // 2
    packed = 3 * half
    slots = n_row * cap
    per_plane = n_row // n_col
    chips_plane = per_plane // 2
    block = width * chunks
    pick0, len0, sig0 = slots, slots + per_dev, slots + 2 * per_dev
    has_left = plane > 0
    has_right = plane < n_col - 1

    share = n_col >= 4
    pieces = chunks
    piece = row_width // pieces
    is_end = ((plane == 0) | (plane == n_col - 1)) & share
    is_helper = ((plane == 1) | (plane == n_col - 2)) & share
    low_half = plane <= n_col - 1 - plane
    end_plane = jnp.where(low_half, 0, n_col - 1)
    helper_plane = jnp.where(low_half, 1, n_col - 2)

    barrier = pltpu.get_barrier_semaphore()
    for other in range(1, n_row):
        pl.semaphore_signal(barrier, inc=1, device_id=((me + other) % n_row, plane), device_id_type=MESH)

    @pl.when(has_left)
    def _():
        pl.semaphore_signal(barrier, inc=1, device_id=(me, plane - 1), device_id_type=MESH)

    @pl.when(has_right)
    def _():
        pl.semaphore_signal(barrier, inc=1, device_id=(me, plane + 1), device_id_type=MESH)

    def selection(p, weighted):
        s = lax.broadcasted_iota(jnp.int32, (packed, 2 * atom_w), 0)
        t = lax.broadcasted_iota(jnp.int32, (packed, 2 * atom_w), 1)
        extra = meta[len0 + 2 * p] - half
        source = jnp.where(
            s < half, s, jnp.where(s < 2 * half, s + half, jnp.where(s - 2 * half < extra, s - half, s + half - extra))
        )
        hit = source == t
        if weighted:
            sig = jnp.where(t < atom_w, meta[sig0 + 2 * p], meta[sig0 + 2 * p + 1])
            hit = hit & (sig > 0)
        return jnp.where(hit, 1.0, 0.0).astype(BF16)

    def pack_coeffs(p, carry):
        rows = coeffs[pl.ds(pl.multiple_of(p * 2 * atom_w, 2 * atom_w), 2 * atom_w), :]
        live = jnp.dot(selection(p, False), rows, preferred_element_type=F32).astype(BF16)
        at = pl.ds(pl.multiple_of(p * packed, 16), packed)
        for k in range(chunks):
            for b in range(per_plane):
                lo = b * block + k * width
                gathered[plane, k, at, b * width : (b + 1) * width] = live[:, lo : lo + width]
        return carry

    lax.fori_loop(0, pairs, pack_coeffs, 0)
    pl.semaphore_wait(barrier, n_row - 1 + has_left.astype(jnp.int32) + has_right.astype(jnp.int32))

    def to_right(z, k):
        return remote(gathered.at[z, k], gathered.at[z, k], r_ss.at[z, k], g_rs.at[z, k], (me, plane + 1))

    def to_left(z, k):
        return remote(gathered.at[z, k], gathered.at[z, k], l_ss.at[z, k], g_rs.at[z, k], (me, plane - 1))

    def goes_right(z):
        ok = (z <= plane) & has_right
        return ok & ((plane != n_col - 2) | (z == plane)) if share else ok

    def goes_left(z):
        ok = (z >= plane) & has_left
        return ok & ((plane != 1) | (z == plane)) if share else ok

    def forward(z, k):
        @pl.when(goes_right(z))
        def _():
            to_right(z, k).start()

        @pl.when(goes_left(z))
        def _():
            to_left(z, k).start()

    for k in range(chunks):
        forward(plane, k)

    def a_copy(owner):
        return remote(asend.at[owner], arecv.at[me], a_ss.at[owner], a_rs.at[me], (owner, plane))

    def place(step, carry):
        owner = (me + step) % n_row

        @pl.when(step > 0)
        def _():
            for c in range(cap):
                asend[owner, c] = integrals[meta[owner * cap + c]]
            a_copy(owner).start()

        @pl.when(step == 0)
        def _():
            for c in range(cap):
                arecv[me, c] = integrals[meta[me * cap + c]]

        return carry

    lax.fori_loop(0, n_row, place, 0)

    def wait_blocks(step, carry):
        source = (me + step) % n_row
        remote(asend.at[source], arecv.at[source], a_ss.at[source], a_rs.at[source], (source, plane)).wait_recv()
        return carry

    lax.fori_loop(1, n_row, wait_blocks, 0)

    def pack_kept(p, carry):
        first, second = meta[pick0 + 2 * p], meta[pick0 + 2 * p + 1]
        rows = jnp.concatenate([arecv[first // cap, first % cap], arecv[second // cap, second % cap]], axis=0)
        live = jnp.dot(selection(p, True), rows, preferred_element_type=F32).astype(BF16)
        kept[pl.ds(pl.multiple_of(p * packed, 16), packed), :] = live
        return carry

    lax.fori_loop(0, pairs, pack_kept, 0)

    def piece_at(q):
        return pl.ds(pl.multiple_of(q * piece, 128), piece)

    def kept_copy(q):
        return remote(
            kept.at[:, piece_at(q)], kept_end.at[:, piece_at(q)], k_ss.at[q], k_rs.at[q], (me, helper_plane)
        )

    if share:

        @pl.when(is_end)
        def _():
            for q in range(pieces):
                kept_copy(q).start()

    def core_copy(z, k):
        return remote(send1.at[z, k], recv1.at[z, k], s1_ss.at[z, k], s1_rs.at[z, k], (partner, plane))

    def chip_copy(target, k):
        return remote(
            mine1.at[target, k], sums.at[chip, k], s2_ss.at[target, k], s2_rs.at[chip, k], (2 * target + core, plane)
        )

    steps = jnp.where(is_end, 2 * chunks, n_col * chunks)

    def finish(n):
        z = nearest(plane, n_col, n // chunks)
        k = n % chunks
        core_copy(z, k).wait_recv()
        for j in range(chips_plane):
            target = z * chips_plane + j
            both = mine1[target, k].astype(F32) + recv1[z, k, j].astype(F32)

            @pl.when(target == chip)
            def _():
                sums[target, k] = both.astype(BF16)

            @pl.when(target != chip)
            def _():
                mine1[target, k] = both.astype(BF16)
                chip_copy(target, k).start()

    near = (n_col - 3) * chunks

    def begin(t):
        return near * t + t * t

    def decode(e):
        e = jnp.asarray(e, jnp.int32)
        t = jnp.int32(0)
        for w in range(1, chunks):
            t += (e >= begin(w)).astype(jnp.int32)
        u = e - begin(t)
        last = u >= near
        v = u - near
        early = v <= t
        far = jnp.where(last, n_col - 3, u // chunks)
        k = jnp.where(last, jnp.where(early, v, t), u % chunks)
        q = jnp.where(last & (v > t), v - 1 - t, t)
        z = jnp.where(low_half, far + 2, n_col - 3 - far)
        return far, z, k, q

    def far_core_copy(far, k, q):
        return remote(
            send4.at[far, k, q], recv4.at[far, k, q], s4_ss.at[far, k, q], s4_rs.at[far, k, q], (partner, plane)
        )

    def far_copy(far, k, q):
        return remote(
            mine4.at[far, k, q], relay.at[far, k, q], s3_ss.at[far, k, q], s3_rs.at[far, k, q], (me, end_plane)
        )

    def relay_copy(far, j, k, q, target):
        return remote(
            relay.at[far, k, q, j], sums.at[chip, k, :, piece_at(q)], s5_ss.at[far, k, q, j], s5_rs.at[chip, k, q],
            (2 * target + core, plane),
        )

    def far_start(e):
        far, z, k, q = decode(e)

        part = lax.dot_general(
            gathered[z, k], kept_end[:, piece_at(q)], (((0,), (0,)), ((), ())), preferred_element_type=F32
        ).astype(BF16)
        for j in range(chips_plane):
            lower = part[2 * j * width : (2 * j + 1) * width]
            upper = part[(2 * j + 1) * width : (2 * j + 2) * width]
            is_lower = core == 0
            mine4[far, k, q, j] = jnp.where(is_lower, lower, upper)
            send4[far, k, q, j] = jnp.where(is_lower, upper, lower)
        far_core_copy(far, k, q).start()

    def far_finish(e):
        far, z, k, q = decode(e)
        far_core_copy(far, k, q).wait_recv()
        for j in range(chips_plane):
            both = mine4[far, k, q, j].astype(F32) + recv4[far, k, q, j].astype(F32)
            mine4[far, k, q, j] = both.astype(BF16)
        far_copy(far, k, q).start()

    def step_body(n, carry):
        @pl.when(n < steps)
        def _():
            z = nearest(plane, n_col, n // chunks)
            k = n % chunks

            @pl.when(z != plane)
            def _():
                to_right(z, k).wait_recv()
                forward(z, k)

            part = lax.dot_general(
                gathered[z, k], kept[...], (((0,), (0,)), ((), ())), preferred_element_type=F32
            ).astype(BF16)
            for j in range(chips_plane):
                lower = part[2 * j * width : (2 * j + 1) * width]
                upper = part[(2 * j + 1) * width : (2 * j + 2) * width]
                is_lower = core == 0
                mine1[z * chips_plane + j, k] = jnp.where(is_lower, lower, upper)
                send1[z, k, j] = jnp.where(is_lower, upper, lower)
            core_copy(z, k).start()

        @pl.when(n > 0)
        def _():
            finish(n - 1)

        if share:
            t = n - (n_col - 1) * chunks

            @pl.when(is_helper & (t >= 0) & (t < chunks))
            def _():
                kept_copy(t).wait_recv()

                def far_body(e, carry):
                    far_start(e)

                    @pl.when(e > 0)
                    def _():
                        far_finish(e - 1)

                    return carry

                lax.fori_loop(begin(t), begin(t + 1), far_body, 0)

        return carry

    lax.fori_loop(0, steps + 1, step_body, 0)
    if share:

        @pl.when(is_helper)
        def _():
            far_finish(begin(chunks) - 1)

        @pl.when(is_end)
        def _():
            def pass_on(e, carry):
                far, z, k, q = decode(e)
                far_copy(far, k, q).wait_recv()
                for j in range(chips_plane):
                    target = z * chips_plane + j

                    @pl.when(target == chip)
                    def _():
                        sums[target, k, :, piece_at(q)] = relay[far, k, q, j]

                    @pl.when(target != chip)
                    def _():
                        relay_copy(far, j, k, q, target).start()

                return carry

            lax.fori_loop(0, begin(chunks), pass_on, 0)

    my_plane = chip // chips_plane
    distance = jnp.where(low_half, my_plane, n_col - 1 - my_plane)
    from_helper = is_end & (distance >= 2)

    @pl.when(jnp.logical_not(from_helper))
    def _():
        def wait_sums(step, carry):
            source = (chip + step) % n_chip
            for k in range(chunks):
                remote(
                    mine1.at[source, k], sums.at[source, k], s2_ss.at[source, k], s2_rs.at[source, k],
                    (2 * source + core, plane),
                ).wait_recv()
            return carry

        lax.fori_loop(1, n_chip, wait_sums, 0)

    if share:

        @pl.when(from_helper)
        def _():
            def wait_far(step, carry):
                source = (chip + step) % n_chip
                for k in range(chunks):
                    for q in range(pieces):
                        remote(
                            relay.at[0, k, q, 0], sums.at[source, k, :, piece_at(q)], s5_ss.at[0, k, q, 0],
                            s5_rs.at[source, k, q], (2 * source + core, plane),
                        ).wait_recv()
                return carry

            lax.fori_loop(1, n_chip, wait_far, 0)

    for k in range(chunks):
        acc = sums[0, k].astype(F32)
        for q in range(1, n_chip):
            acc += sums[q, k].astype(F32)
        out[k * width : (k + 1) * width, :] = acc.astype(BF16)

    def drain_blocks(step, carry):
        a_copy((me + step) % n_row).wait_send()
        return carry

    lax.fori_loop(1, n_row, drain_blocks, 0)

    def drain(n, carry):
        z, k = nearest(plane, n_col, n // chunks), n % chunks
        core_copy(z, k).wait_send()

        @pl.when(goes_right(z))
        def _():
            to_right(z, k).wait_send()

        @pl.when(goes_left(z))
        def _():
            to_left(z, k).wait_send()

        for j in range(chips_plane):
            target = z * chips_plane + j

            @pl.when(target != chip)
            def _():
                chip_copy(target, k).wait_send()

        return carry

    lax.fori_loop(0, steps, drain, 0)
    if share:

        @pl.when(is_end)
        def _():
            for q in range(pieces):
                kept_copy(q).wait_send()

            def drain_relay(e, carry):
                far, z, k, q = decode(e)
                for j in range(chips_plane):
                    target = z * chips_plane + j

                    @pl.when(target != chip)
                    def _():
                        relay_copy(far, j, k, q, target).wait_send()

                return carry

            lax.fori_loop(0, begin(chunks), drain_relay, 0)

        @pl.when(is_helper)
        def _():
            def drain_far(e, carry):
                far, z, k, q = decode(e)
                far_core_copy(far, k, q).wait_send()
                far_copy(far, k, q).wait_send()
                return carry

            lax.fori_loop(0, begin(chunks), drain_far, 0)


def body(integrals, coeffs, mask, offsets, atom_of_slot):
    n_row = lax.axis_size("row")
    n_col = lax.axis_size("col")
    me = lax.axis_index("row")
    plane = lax.axis_index("col")
    per_dev, atom_w, row_width = integrals.shape
    rows, cols = coeffs.shape
    cap = max(2, -(-per_dev // n_row))
    slots = n_row * cap
    block = cols * n_col // n_row
    chunks = max(1, min(4, block // 128))
    width = block // chunks
    per_plane = n_row // n_col

    holders = atom_of_slot.reshape(n_row, per_dev)
    slot = jnp.arange(per_dev, dtype=jnp.int32)
    mine = lax.dynamic_slice_in_dim(atom_of_slot, me * per_dev, per_dev)
    owner = mine // per_dev
    before = (owner[None, :] == owner[:, None]) & (slot[None, :] < slot[:, None])
    position = owner * cap + jnp.sum(before.astype(jnp.int32), axis=1)
    order = jnp.sum(
        jnp.where(jnp.arange(slots, dtype=jnp.int32)[:, None] == position[None, :], slot[None, :], 0), axis=1
    )
    is_mine = holders // per_dev == me
    earlier = is_mine[:, None, :] & (slot[None, None, :] < slot[None, :, None])
    arrival = jnp.sum(earlier.astype(jnp.int32), axis=2)
    place = (jnp.arange(n_row, dtype=jnp.int32)[:, None] * cap + arrival).reshape(-1)
    pick = jnp.sum(
        jnp.where((me * per_dev + slot)[:, None] == atom_of_slot[None, :], place[None, :], 0), axis=1
    )
    bounds = lax.dynamic_slice_in_dim(offsets, me * per_dev, per_dev + 1)
    lengths = bounds[1:] - bounds[:-1]
    significant = lax.dynamic_slice(mask, (me * per_dev, plane), (per_dev, 1))[:, 0]
    meta = jnp.concatenate([order, pick, lengths, significant])

    packed = rows * 3 // 4
    dma = pltpu.SemaphoreType.DMA
    n_chip = n_row // 2
    pair_width = per_plane * width
    n_far = max(1, n_col - 2)
    far_shape = (n_far, chunks, chunks, per_plane // 2, width, row_width // chunks)
    return pl.pallas_call(
        functools.partial(kernel, n_row, n_col, cap, chunks, width),
        out_shape=jax.ShapeDtypeStruct((block, row_width), BF16),
        in_specs=[pl.BlockSpec(memory_space=pltpu.SMEM)] + [pl.BlockSpec(memory_space=pltpu.VMEM)] * 2,
        out_specs=pl.BlockSpec(memory_space=pltpu.VMEM),
        scratch_shapes=[
            pltpu.VMEM((n_row, cap, atom_w, row_width), BF16),
            pltpu.VMEM((n_row, cap, atom_w, row_width), BF16),
            pltpu.VMEM((packed, row_width), BF16),
            pltpu.VMEM((n_col, chunks, packed, pair_width), BF16),
            pltpu.VMEM((n_chip, chunks, width, row_width), BF16),
            pltpu.VMEM((n_col, chunks, per_plane // 2, width, row_width), BF16),
            pltpu.VMEM((n_col, chunks, per_plane // 2, width, row_width), BF16),
            pltpu.VMEM((n_chip, chunks, width, row_width), BF16),
            pltpu.VMEM((packed, row_width), BF16),
            pltpu.VMEM(far_shape, BF16),
            pltpu.VMEM(far_shape, BF16),
            pltpu.VMEM(far_shape, BF16),
            pltpu.VMEM(far_shape, BF16),
            dma((n_row,)),
            dma((n_row,)),
            dma((n_col, chunks)),
            dma((n_col, chunks)),
            dma((n_col, chunks)),
            dma((n_col, chunks)),
            dma((n_col, chunks)),
            dma((n_chip, chunks)),
            dma((n_chip, chunks)),
            dma((chunks,)),
            dma((chunks,)),
            dma((n_far, chunks, chunks)),
            dma((n_far, chunks, chunks)),
            dma((n_far, chunks, chunks)),
            dma((n_far, chunks, chunks)),
            dma((n_far, chunks, chunks, per_plane // 2)),
            dma((n_chip, chunks, chunks)),
        ],
        compiler_params=pltpu.CompilerParams(
            collective_id=0, has_side_effects=True, vmem_limit_bytes=62 << 20
        ),
    )(meta, integrals, coeffs)


def solution(mesh):
    in_specs = (P("row", None, "col"), P("row", "col"), P(), P(), P())
    out_specs = P("row", "col")
    return jax.shard_map(body, mesh=mesh, in_specs=in_specs, out_specs=out_specs, check_vma=False)
```
